32 devices in a mesh: graph: 8 (over z, x), mp: 4 (over y, core).
Axes of the slice: x: 2, y: 2, z: 4, core: 2. Of those that a mesh axis runs over, the one named last changes fastest.
Arguments:
- edge_state: bfloat16 [4096, 1536], P('graph', 'mp'), may hold values from -6 to 6
- down_weight: bfloat16 [1536, 384], P('mp'), may hold values from -0.15625 to 0.15625
- basis: float32 [42, 131072], P(None, ('graph', 'mp')), may hold values from -6 to 6
- basis_weight: float32 [42, 384], replicated, may hold values from -1 to 1
- up_weight: bfloat16 [384, 1536], P(None, 'mp'), may hold values from -0.3125 to 0.3125
- dense_weight: bfloat16 [3, 2, 1536, 1536], P(None, None, None, 'mp'), may hold values from -0.15625 to 0.15625
- send_rows: int32 [8, 32, 64], P('graph', 'mp'), may hold values from 0 to 512, as said below
- trip_in: int32 [131072], P(('graph', 'mp')), may hold values from 0 to 511, as said below
- trip_out: int32 [131072], P(('graph', 'mp')), may hold values from 0 to 511, as said below
- trip_live: int32 [131072], P(('graph', 'mp')), may hold values from 0 to 1, as said below
- edge_atom: int32 [4096], P('graph'), may hold values from 0 to 255
Outputs:
- edge_out: bfloat16 [4096, 1536], P('graph', 'mp')
- atom_out: bfloat16 [256, 1536], P('graph', 'mp')
The draws below stay inside these ranges and needn't reach their ends.
Inputs may be any that keep to these rules, and one draw needn't show every extreme that they name: `send_rows`: entry [s, m * 8 + g, c] is a row among the 512 edges of graph index s listed in slot c for the device at graph index g and mp index m, or 512 for an empty slot; used slots come first in each list, and some device has every list full. `trip_in`: A slot s * 64 + c of the triplet's own device whose list entry from graph index s is used. `trip_out`: A slot s * 64 + c of the triplet's own device whose list entry from graph index s is used. `trip_live`: on each device the real triplets come first; some device has no padding.
All inputs are finite; a program needn't handle non-finite values.
Results may differ from the reference program's by a relative error of at most 0.014.
Values may be sent and summed in bfloat16 or wider, within the bound.
A program may use at most 128 MiB of HBM per device.

```python
import jax
import jax.numpy as jnp
from jax import lax

D = 1536
TRIP = 384
NSBF = 42
TILE = 128
LAYERS = 3
EDGE_DEV = 512
CAP = 64
TILES_DEV = 32
EDGES = 4096
ATOMS = 256
TRIPLETS = 131072
N_GRAPH = 8
N_MP = 4


def list_counts(key):
    count_key = jax.random.fold_in(key, 1701)
    counts = jax.random.randint(count_key, (N_GRAPH * N_MP, N_GRAPH), 1, CAP + 1)
    return counts.at[0].set(CAP)


def draw_send_rows(key, part):
    counts = list_counts(key)
    shaped = counts.reshape(N_GRAPH, N_MP, N_GRAPH).transpose(2, 1, 0).reshape(N_GRAPH, N_MP * N_GRAPH)
    start_rows = jax.random.randint(jax.random.fold_in(key, 2203), (N_GRAPH, N_MP * N_GRAPH), 0, EDGE_DEV)
    position = jnp.arange(CAP, dtype=jnp.int32)
    rows = (start_rows[:, :, None] + position) % EDGE_DEV
    return jnp.where(position < shaped[:, :, None], rows, EDGE_DEV).astype(jnp.int32)


def slot_draw(key, salt):
    counts = list_counts(key)
    per_device = TILES_DEV * TILE
    source = jax.random.randint(jax.random.fold_in(key, salt), (N_GRAPH * N_MP, per_device), 0, N_GRAPH)
    raw = jax.random.randint(jax.random.fold_in(key, salt + 1), (N_GRAPH * N_MP, per_device), 0, 1048576)
    limit = jnp.take_along_axis(counts, source, axis=1)
    return (source * CAP + raw % limit).reshape(-1).astype(jnp.int32)


def draw_trip_in(key, part):
    return slot_draw(key, 3301)


def draw_trip_out(key, part):
    return slot_draw(key, 4409)


def draw_trip_live(key, part):
    per_device = TILES_DEV * TILE
    live_count = jax.random.randint(jax.random.fold_in(key, 5507), (N_GRAPH * N_MP,), per_device // 4, per_device + 1)
    live_count = live_count.at[0].set(per_device)
    position = jnp.arange(per_device, dtype=jnp.int32)
    return (position[None, :] < live_count[:, None]).reshape(-1).astype(jnp.int32)


def place_ends(result, stream_key, smallest, largest):
    shape = result.shape
    place = [jax.random.randint(jax.random.fold_in(stream_key, axis), (), 0, shape[axis]) for axis in range(len(shape))]
    result = result.at[tuple(place)].set(smallest)
    longest = shape.index(max(shape))
    place[longest] = (place[longest] + 1) % shape[longest]
    return result.at[tuple(place)].set(largest)


def levels(key, shape, split, smallest, high):
    def one(dim, blocks):
        draws = jax.random.uniform(jax.random.fold_in(jax.random.fold_in(key, 6), dim), (blocks,), jnp.float32, smallest / len(split), high / len(split))
        return jnp.repeat(jnp.exp(draws), shape[dim] // blocks).reshape((-1,) + (1,) * (len(shape) - dim - 1))

    loudness = one(*split[0])
    for cut in split[1:]:
        loudness = loudness * one(*cut)
    return loudness


def normal_values(key, shape, deviation, most, pieces=(), kind=jnp.bfloat16):
    factor_of = levels(key, shape, pieces, -0.22, 0.18) if pieces else 1.0
    entries = jax.random.normal(key, shape, jnp.float32) * deviation * factor_of
    return jnp.minimum(jnp.maximum(entries, -most), most).astype(kind)


def setup_inputs(seed: int = 0) -> dict:
    streams_of = jax.random.split(jax.random.key(seed), 12)
    edge_state = normal_values(streams_of[0], (EDGES, D), 1.0, 6.0, ((0, 8), (1, 4)))
    down_weight = normal_values(streams_of[1], (D, TRIP), D ** -0.5, 0.15625, ((0, 4),))
    basis = normal_values(streams_of[2], (NSBF, TRIPLETS), 1.0, 6.0, ((1, 32),), jnp.float32)
    basis_weight = normal_values(streams_of[3], (NSBF, TRIP), NSBF ** -0.5, 1.0, (), jnp.float32)
    up_weight = normal_values(streams_of[4], (TRIP, D), TRIP ** -0.5, 0.3125, ((1, 4),))
    dense_weight = normal_values(streams_of[5], (LAYERS, 2, D, D), D ** -0.5, 0.15625, ((3, 4),))
    send_rows = draw_send_rows(jax.random.fold_in(streams_of[11], 71), 0)
    trip_in = draw_trip_in(jax.random.fold_in(streams_of[11], 71), 0)
    trip_out = draw_trip_out(jax.random.fold_in(streams_of[11], 71), 0)
    trip_live = draw_trip_live(jax.random.fold_in(streams_of[11], 71), 0)
    edge_atom = place_ends(jax.random.randint(streams_of[10], (EDGES,), 0, ATOMS), jax.random.fold_in(streams_of[10], 1), 0, ATOMS - 1).astype(jnp.int32)
    return {"edge_state": edge_state, "down_weight": down_weight, "basis": basis, "basis_weight": basis_weight, "up_weight": up_weight, "dense_weight": dense_weight, "send_rows": send_rows, "trip_in": trip_in, "trip_out": trip_out, "trip_live": trip_live, "edge_atom": edge_atom}


inv_root_two = 0.7071067811865476
atom_scale = 0.2


def reference(edge_state, down_weight, basis, basis_weight, up_weight, dense_weight, send_rows, trip_in, trip_out, trip_live, edge_atom):
    projected = jnp.dot(edge_state, down_weight, preferred_element_type=jnp.float32).astype(jnp.bfloat16)
    per_device = TILES_DEV * TILE
    slot_count = N_GRAPH * CAP
    sources = (jnp.arange(N_GRAPH, dtype=jnp.int32) * EDGE_DEV)[:, None]

    def visit(carry, device):
        graph_index = device // N_MP
        mp_index = device % N_MP
        row_lists = lax.dynamic_index_in_dim(send_rows, (mp_index * N_GRAPH + graph_index).astype(jnp.int32), 1, keepdims=False)
        valid_flat = (row_lists < EDGE_DEV).reshape(-1)
        global_rows = (sources + jnp.minimum(row_lists, EDGE_DEV - 1)).reshape(-1).astype(jnp.int32)
        received = jnp.where(valid_flat[:, None], jnp.take(projected, global_rows, axis=0), jnp.zeros((), jnp.bfloat16))
        offset = (device * per_device).astype(jnp.int32)
        basis_part = lax.dynamic_slice_in_dim(basis, offset, per_device, 1)
        in_part = lax.dynamic_slice_in_dim(trip_in, offset, per_device, 0)
        out_part = lax.dynamic_slice_in_dim(trip_out, offset, per_device, 0)
        live_part = lax.dynamic_slice_in_dim(trip_live, offset, per_device, 0)
        angle_coef = lax.dot_general(basis_part, basis_weight, (((0,), (0,)), ((), ())), precision=lax.Precision.HIGHEST, preferred_element_type=jnp.float32)
        trip_values = jnp.take(received, in_part, axis=0).astype(jnp.float32) * angle_coef * live_part[:, None].astype(jnp.float32)
        slot_sums = jax.ops.segment_sum(trip_values, out_part, num_segments=slot_count).astype(jnp.bfloat16)
        contrib = jnp.where(valid_flat[:, None], slot_sums.astype(jnp.float32), jnp.zeros((), jnp.float32))
        carry = carry.at[global_rows].add(contrib)
        return carry, None

    edge_update, _ = lax.scan(visit, jnp.zeros((EDGES, TRIP), jnp.float32), jnp.arange(N_GRAPH * N_MP, dtype=jnp.int32))
    update_rows = edge_update.astype(jnp.bfloat16)
    hidden = edge_state.astype(jnp.float32) + jnp.dot(update_rows, up_weight, preferred_element_type=jnp.float32)
    for layer_index in range(LAYERS):
        inner = jax.nn.silu(jnp.dot(hidden.astype(jnp.bfloat16), dense_weight[layer_index, 0], preferred_element_type=jnp.float32)).astype(jnp.bfloat16)
        outer = jax.nn.silu(jnp.dot(inner, dense_weight[layer_index, 1], preferred_element_type=jnp.float32))
        hidden = (hidden + outer) * inv_root_two
    atom_sum = jax.ops.segment_sum(hidden, edge_atom, num_segments=ATOMS)
    atom_out = jax.nn.silu(atom_scale * atom_sum).astype(jnp.bfloat16)
    edge_out = (hidden + jnp.take(atom_out, edge_atom, axis=0).astype(jnp.float32)).astype(jnp.bfloat16)
    return (edge_out, atom_out)
```

```python
import functools

import jax
import jax.numpy as jnp
from jax import lax
from jax.experimental import pallas as pl
from jax.experimental.pallas import tpu as pltpu
from jax.sharding import PartitionSpec as P

ATOM_DEV = 32
CHUNKS = 4

inv_root_two = 0.7071067811865476
atom_scale = 0.2

MESH = pl.DeviceIdType.MESH
bf16 = jnp.bfloat16
f32 = jnp.float32


def silu(v):
    return v / (1.0 + jnp.exp(-v))


def flip(index, bit):
    return index + bit - 2 * bit * ((index // bit) % 2)


def one_hot(rows, ids):
    shape = (rows, ids.shape[1])
    return jnp.where(lax.broadcasted_iota(jnp.int32, shape, 0) == ids, 1.0, 0.0).astype(bf16)


def dot(a, b, ca=1, cb=0):
    return lax.dot_general(a, b, (((ca,), (cb,)), ((), ())), preferred_element_type=f32)


def gather_plan(mp):
    plan, held, bit = [], [0], mp // 2
    while bit >= 1:
        plan += [(bit, off) for off in held]
        held += [bit ^ off for off in held]
        bit //= 2
    return plan, held


def kernel(
    graph, mp, tile,
    state_ref, down_ref, basis_ref, bw_ref, up_ref, dense_hbm, lists_ref, in_ref, out_ref, live_ref, atom_ref,
    edge_out_ref, atom_out_ref,
    weight, weight_sem,
    part_a, got_a, sum_a, more_a, full_a,
    part_b, got_b, sum_b, more_b, full_b,
    red_send, red_recv,
    to_a, from_a, to_b, from_b, xc_send, xc_recv,
    recv_t, angle, slots,
    acts, hidden, act_send, act_recv,
    atoms_own, atoms_to, atoms_from, table,
    bar_dummy,
):
    g = lax.axis_index("graph")
    m = lax.axis_index("mp")
    rows, width = state_ref.shape
    trip = down_ref.shape[1]
    layers = weight.shape[0] // 2
    slot_total = slots.shape[0]
    cap = slot_total // graph
    triplets = in_ref.shape[1]
    atoms = graph * ATOM_DEV
    half = rows // 2
    bits = [1 << i for i in range(mp.bit_length() - 1)]

    load = pltpu.make_async_copy(dense_hbm, weight, weight_sem)
    load.start()

    barrier = pltpu.get_barrier_semaphore()

    def greet(k, _):
        pl.semaphore_signal(barrier, inc=1, device_id={"graph": (g + k) % graph}, device_id_type=MESH)
        return 0

    lax.fori_loop(1, graph, greet, 0)
    for bit in bits:
        pl.semaphore_signal(barrier, inc=1, device_id={"mp": flip(m, bit)}, device_id_type=MESH)

    def mp_copy(src, dst, which, slot, bit):
        return pltpu.make_async_remote_copy(
            src_ref=src, dst_ref=dst, send_sem=red_send.at[which, slot], recv_sem=red_recv.at[which, slot],
            device_id={"mp": flip(m, bit)}, device_id_type=MESH)

    mine = pl.multiple_of((m % 2) * half, half)
    other = pl.multiple_of(half - (m % 2) * half, half)

    def mp_sum(which, part, got, summed, more, full):
        first = mp_copy(part.at[pl.ds(other, half)], got, which, 0, 1)
        first.start()
        first.wait()
        total = part[pl.ds(mine, half)].astype(f32) + got[...].astype(f32)
        for i, bit in enumerate(bits[1:]):
            summed[i] = total.astype(bf16)
            step = mp_copy(summed.at[i], more.at[i], which, 1 + i, bit)
            step.start()
            step.wait()
            total = summed[i].astype(f32) + more[i].astype(f32)
        full[pl.ds(mine, half)] = total.astype(bf16)
        last = mp_copy(full.at[pl.ds(mine, half)], full.at[pl.ds(mine, half)], which, len(bits), 1)
        last.start()
        last.wait()

    def exchange(which, src_at, dst, dst_at, size):
        def copy(k):
            peer = (g + k) % graph
            return pltpu.make_async_remote_copy(
                src_ref=src_at(peer), dst_ref=dst_at(g),
                send_sem=xc_send.at[which, k], recv_sem=xc_recv.at[which, k],
                device_id={"graph": peer}, device_id_type=MESH)

        def start(k, _):
            copy(k).start()
            return 0

        def wait(k, _):
            copy(k).wait()
            return 0

        return (lambda: lax.fori_loop(1, graph, start, 0)), (lambda: lax.fori_loop(1, graph, wait, 0))

    def block(ref, size):
        return lambda i: ref.at[pl.ds(pl.multiple_of(i * size, size), size)]

    part_a[...] = dot(state_ref[...], down_ref[...]).astype(bf16)
    pl.semaphore_wait(barrier, graph - 1 + len(bits))
    mp_sum(0, part_a, got_a, sum_a, more_a, full_a)

    step_rows = min(slot_total, 512)
    own = pl.ds(pl.multiple_of(g * cap, cap), cap)

    def pick(i, _):
        at = pl.ds(pl.multiple_of(i * step_rows, step_rows), step_rows)
        lists = one_hot(rows, lists_ref[:, at])
        to_a[at, :] = dot(lists, full_a[...], 0, 0).astype(bf16)
        return 0

    lax.fori_loop(0, slot_total // step_rows, pick, 0)
    start, wait = exchange(0, block(to_a, cap), from_a, block(from_a, cap), cap)
    start()
    from_a[own] = to_a[own]

    def angles(i, _):
        at = pl.ds(pl.multiple_of(i * tile, tile), tile)
        angle[:, at] = lax.dot_general(
            bw_ref[...], basis_ref[:, at], (((1,), (0,)), ((), ())),
            precision=lax.Precision.HIGHEST, preferred_element_type=f32)
        return 0

    lax.fori_loop(0, triplets // tile, angles, 0)
    slots[...] = jnp.zeros_like(slots)
    wait()

    recv_t[...] = from_a[...].astype(f32).T.astype(bf16)

    def trips(i, _):
        at = pl.ds(pl.multiple_of(i * tile, tile), tile)
        source = one_hot(slot_total, in_ref[:, at])
        value = dot(recv_t[...], source) * angle[:, at]
        target = one_hot(slot_total, jnp.where(live_ref[:, at] > 0, out_ref[:, at], -1))
        slots[...] += dot(target, value.astype(bf16), 1, 1)
        return 0

    lax.fori_loop(0, triplets // tile, trips, 0)
    to_b[...] = slots[...].astype(bf16)

    start, wait = exchange(1, block(to_b, cap), from_b, block(from_b, cap), cap)
    start()
    from_b[own] = to_b[own]
    wait()

    def put(i, total):
        at = pl.ds(pl.multiple_of(i * step_rows, step_rows), step_rows)
        return total + dot(one_hot(rows, lists_ref[:, at]), from_b[at, :])

    if slot_total == step_rows:
        part_b[...] = dot(one_hot(rows, lists_ref[...]), from_b[...]).astype(bf16)
    else:
        hidden[:, :trip] = jnp.zeros((rows, trip), f32)

        def put(i, _):
            at = pl.ds(pl.multiple_of(i * step_rows, step_rows), step_rows)
            hidden[:, :trip] += dot(one_hot(rows, lists_ref[:, at]), from_b[at, :])
            return 0

        lax.fori_loop(0, slot_total // step_rows, put, 0)
        part_b[...] = hidden[:, :trip].astype(bf16)
    mp_sum(1, part_b, got_b, sum_b, more_b, full_b)

    plan, held = gather_plan(mp)
    size = rows // CHUNKS

    def other_of(off):
        index = m
        for bit in bits:
            if off & bit:
                index = flip(index, bit)
        return index

    def act_copy(layer, c, which):
        bit, off = plan[which]
        at = acts.at[layer, other_of(off), pl.ds(c * size, size)]
        return pltpu.make_async_remote_copy(
            src_ref=at, dst_ref=at,
            send_sem=act_send.at[layer, c, which], recv_sem=act_recv.at[layer, c, which],
            device_id={"mp": flip(m, bit)}, device_id_type=MESH)

    local = [i for i, (bit, off) in enumerate(plan) if off == 0]
    relayed = [i for i, (bit, off) in enumerate(plan) if off != 0]
    brings = {bit ^ off: i for i, (bit, off) in enumerate(plan)}
    relays_from = sorted({brings[plan[i][1]] for i in relayed})

    def send(layer, c):
        for i in local:
            act_copy(layer, c, i).start()

    def relay(layer, c):
        for i in relayed:
            first = brings[plan[i][1]]
            if [j for j in relayed if brings[plan[j][1]] == first][0] == i:
                act_copy(layer, c, first).wait_recv()
            act_copy(layer, c, i).start()

    def finish(layer, c):
        for i in range(len(plan)):
            if i not in relays_from:
                act_copy(layer, c, i).wait_recv()

    for c in range(CHUNKS):
        at = pl.ds(c * size, size)
        first = state_ref[at, :].astype(f32) + dot(full_b[at, :], up_ref[...])
        hidden[at, :] = first
        acts[0, m, at, :] = first.astype(bf16)
        send(0, c)

    load.wait()
    relay(0, 0)

    def layer_step(l, _):
        for inside in range(2):
            k = 2 * l + inside
            for c in range(CHUNKS):
                at = pl.ds(c * size, size)
                if c + 1 < CHUNKS:
                    relay(k, c + 1)
                elif inside == 0:
                    relay(k + 1, 0)
                else:
                    @pl.when(l + 1 < layers)
                    def _():
                        relay(k + 1, 0)
                finish(k, c)
                total = None
                for off in held:
                    index = other_of(off)
                    term = dot(acts[k, index, at, :], weight[k, pl.ds(pl.multiple_of(index * width, width), width), :])
                    total = term if total is None else total + term
                value = silu(total)
                if inside == 0:
                    acts[k + 1, m, at, :] = value.astype(bf16)
                    send(k + 1, c)
                else:
                    value = (hidden[at, :] + value) * inv_root_two
                    hidden[at, :] = value

                    @pl.when(l + 1 < layers)
                    def _():
                        acts[k + 1, m, at, :] = value.astype(bf16)
                        send(k + 1, c)
        return 0

    lax.fori_loop(0, layers, layer_step, 0)

    atom_rows = min(atoms, 256)

    def collect(i, _):
        at = pl.ds(pl.multiple_of(i * atom_rows, atom_rows), atom_rows)
        ids = one_hot(atom_rows, atom_ref[...] - i * atom_rows)
        high = hidden[...].astype(bf16)
        low = (hidden[...] - high.astype(f32)).astype(bf16)
        total = dot(ids, high) + dot(ids, low)
        atoms_own[at, :] = total
        atoms_to[at, :] = total.astype(bf16)
        return 0

    lax.fori_loop(0, atoms // atom_rows, collect, 0)
    start, wait = exchange(2, block(atoms_to, ATOM_DEV), atoms_from, block(atoms_from, ATOM_DEV), ATOM_DEV)
    start()
    here = pl.ds(pl.multiple_of(g * ATOM_DEV, ATOM_DEV), ATOM_DEV)
    atoms_from[here] = jnp.zeros((ATOM_DEV, width), bf16)
    wait()

    def add(i, total):
        return total + atoms_from[pl.ds(pl.multiple_of(i * ATOM_DEV, ATOM_DEV), ATOM_DEV)].astype(f32)

    total = lax.fori_loop(0, graph, add, atoms_own[here])
    mine_out = silu(atom_scale * total).astype(bf16)
    table[here] = mine_out
    atom_out_ref[...] = mine_out
    start, wait = exchange(3, lambda peer: block(table, ATOM_DEV)(g), table, block(table, ATOM_DEV), ATOM_DEV)
    start()

    def drain(k, _):
        for c in range(CHUNKS):
            for i in range(len(plan)):
                act_copy(k, c, i).wait_send()
        return 0

    lax.fori_loop(0, 2 * layers, drain, 0)
    wait()

    def spread(i, _):
        at = pl.ds(pl.multiple_of(i * atom_rows, atom_rows), atom_rows)
        hidden[...] += dot(one_hot(atom_rows, atom_ref[...] - i * atom_rows), table[at, :], 0, 0)
        return 0

    lax.fori_loop(0, atoms // atom_rows, spread, 0)
    edge_out_ref[...] = hidden[...].astype(bf16)


def local(graph, mp, edge_state, down_weight, basis, basis_weight, up_weight, dense_weight,
          send_rows, trip_in, trip_out, trip_live, edge_atom):
    rows, width = edge_state.shape
    trip = down_weight.shape[1]
    slot_total = graph * send_rows.shape[2]
    triplets = trip_in.shape[0]
    maps = dense_weight.shape[0] * dense_weight.shape[1]
    tile = 512 if slot_total <= 512 else 128
    atoms = graph * ATOM_DEV
    stages = mp.bit_length()
    extra = max(stages - 2, 1)
    half = rows // 2
    vmem = pltpu.VMEM
    reduce_bufs = [
        vmem((rows, trip), bf16), vmem((half, trip), bf16), vmem((extra, half, trip), bf16),
        vmem((extra, half, trip), bf16), vmem((rows, trip), bf16),
    ]
    dma = pltpu.SemaphoreType.DMA
    spec = pl.BlockSpec(memory_space=pltpu.VMEM)
    return pl.pallas_call(
        functools.partial(kernel, graph, mp, tile),
        out_shape=(
            jax.ShapeDtypeStruct((rows, width), bf16),
            jax.ShapeDtypeStruct((ATOM_DEV, width), bf16),
        ),
        in_specs=[spec] * 5 + [pl.BlockSpec(memory_space=pl.ANY)] + [spec] * 5,
        out_specs=(spec, spec),
        scratch_shapes=[
            vmem((maps,) + dense_weight.shape[2:], bf16), dma(()),
            *reduce_bufs, *reduce_bufs,
            dma((2, stages)), dma((2, stages)),
            vmem((slot_total, trip), bf16), vmem((slot_total, trip), bf16),
            vmem((slot_total, trip), bf16), vmem((slot_total, trip), bf16),
            dma((4, graph)), dma((4, graph)),
            vmem((trip, slot_total), bf16), vmem((trip, triplets), f32), vmem((slot_total, trip), f32),
            vmem((maps, mp, rows, width), bf16), vmem((rows, max(width, trip)), f32),
            dma((maps, CHUNKS, mp - 1)), dma((maps, CHUNKS, mp - 1)),
            vmem((atoms, width), f32), vmem((atoms, width), bf16), vmem((atoms, width), bf16),
            vmem((atoms, width), bf16),
            vmem((8, 128), f32),
        ],
        compiler_params=pltpu.CompilerParams(
            collective_id=0, has_side_effects=True, vmem_limit_bytes=64000 * 1024
        ),
        name="edge_block",
    )(
        edge_state, down_weight, basis, basis_weight.T, up_weight,
        dense_weight.reshape((maps,) + dense_weight.shape[2:]),
        send_rows.reshape(1, slot_total), trip_in.reshape(1, triplets), trip_out.reshape(1, triplets),
        trip_live.reshape(1, triplets), edge_atom.reshape(1, rows),
    )


def solution(mesh):
    in_specs = (
        P("graph", "mp"),
        P("mp", None),
        P(None, ("graph", "mp")),
        P(),
        P(None, "mp"),
        P(None, None, None, "mp"),
        P("graph", "mp", None),
        P(("graph", "mp")),
        P(("graph", "mp")),
        P(("graph", "mp")),
        P("graph"),
    )
    out_specs = (P("graph", "mp"), P("graph", "mp"))
    body = functools.partial(local, mesh.shape["graph"], mesh.shape["mp"])
    return jax.shard_map(body, mesh=mesh, in_specs=in_specs, out_specs=out_specs, check_vma=False)
```

```python
import functools

import jax
import jax.numpy as jnp
from jax import lax
from jax.experimental import pallas as pl
from jax.experimental.pallas import tpu as pltpu
from jax.sharding import PartitionSpec as P

ATOM_DEV = 32
CHUNKS = 4

inv_root_two = 0.7071067811865476
atom_scale = 0.2

MESH = pl.DeviceIdType.MESH
bf16 = jnp.bfloat16
f32 = jnp.float32


def silu(v):
    return v / (1.0 + jnp.exp(-v))


def flip(index, bit):
    return index + bit - 2 * bit * ((index // bit) % 2)


def one_hot(rows, ids):
    shape = (rows, ids.shape[1])
    return jnp.where(lax.broadcasted_iota(jnp.int32, shape, 0) == ids, 1.0, 0.0).astype(bf16)


def dot(a, b, ca=1, cb=0):
    return lax.dot_general(a, b, (((ca,), (cb,)), ((), ())), preferred_element_type=f32)


def gather_plan(mp):
    plan, held, bit = [], [0], mp // 2
    while bit >= 1:
        plan += [(bit, off) for off in held]
        held += [bit ^ off for off in held]
        bit //= 2
    return plan, held


def kernel(
    graph, mp, tile,
    state_ref, down_ref, basis_ref, bw_ref, up_ref, dense_hbm, lists_ref, in_ref, out_ref, live_ref, atom_ref,
    edge_out_ref, atom_out_ref,
    weight, weight_sem,
    part_a, got_a, sum_a, more_a, full_a,
    part_b, got_b, sum_b, more_b, full_b,
    red_send, red_recv,
    to_a, from_a, to_b, from_b, xc_send, xc_recv,
    lists_flat, list_hot, angle, slots, in_hot, out_hot,
    acts, hidden, act_send, act_recv,
    atoms_own, atoms_to, atoms_from, table,
):
    g = lax.axis_index("graph")
    m = lax.axis_index("mp")
    rows, width = state_ref.shape
    trip = down_ref.shape[1]
    layers = weight.shape[0] // 2
    cap = lists_ref.shape[2]
    slot_total = graph * cap
    pieces, lane = to_a.shape[0], to_a.shape[2]
    kept = in_hot is not None
    triplets = in_ref.shape[1]
    atoms = graph * ATOM_DEV
    half = rows // 2
    bits = [1 << i for i in range(mp.bit_length() - 1)]

    load = pltpu.make_async_copy(dense_hbm, weight, weight_sem)
    load.start()

    barrier = pltpu.get_barrier_semaphore()

    def greet(k, _):
        pl.semaphore_signal(barrier, inc=1, device_id={"graph": (g + k) % graph}, device_id_type=MESH)
        return 0

    lax.fori_loop(1, graph, greet, 0)
    for bit in bits:
        pl.semaphore_signal(barrier, inc=1, device_id={"mp": flip(m, bit)}, device_id_type=MESH)

    def mp_copy(src, dst, which, slot, i, bit):
        return pltpu.make_async_remote_copy(
            src_ref=src, dst_ref=dst, send_sem=red_send.at[which, slot, i], recv_sem=red_recv.at[which, slot, i],
            device_id={"mp": flip(m, bit)}, device_id_type=MESH)

    mine = pl.multiple_of((m % 2) * half, half)
    other = pl.multiple_of(half - (m % 2) * half, half)
    size = rows // CHUNKS
    subs = range(CHUNKS // 2)

    def mp_sum(which, part, got, summed, more, full, meanwhile=None, ready=None):
        at = [pl.ds(i * size, size) for i in subs]
        firsts = [mp_copy(part.at[pl.ds(other + i * size, size)], got.at[at[i]], which, 0, i, 1) for i in subs]
        steps = [[mp_copy(summed.at[b, at[i]], more.at[b, at[i]], which, 1 + b, i, bit) for i in subs]
                 for b, bit in enumerate(bits[1:])]
        for first in firsts:
            first.start()

        def total(b, i):
            if b == 0:
                return part[pl.ds(mine + i * size, size)].astype(f32) + got[at[i]].astype(f32)
            return summed[b - 1, at[i]].astype(f32) + more[b - 1, at[i]].astype(f32)

        for b in range(len(bits) - 1):
            for i in subs:
                (firsts[i] if b == 0 else steps[b - 1][i]).wait()
                summed[b, at[i]] = total(b, i).astype(bf16)
                steps[b][i].start()
        if meanwhile is not None:
            meanwhile()
        lasts = []
        for i in subs:
            (firsts[i] if len(bits) == 1 else steps[-1][i]).wait()
            here = pl.ds(mine + i * size, size)
            full[here] = total(len(bits) - 1, i).astype(bf16)
            lasts.append(mp_copy(full.at[here], full.at[here], which, len(bits), i, 1))
            lasts[i].start()
            if ready is not None:
                lasts[i].wait()
                ready(i)
        if ready is None:
            for last in lasts:
                last.wait()

    def exchange(which, src_at, dst, dst_at, size):
        def copy(k):
            peer = (g + k) % graph
            return pltpu.make_async_remote_copy(
                src_ref=src_at(peer), dst_ref=dst_at(g),
                send_sem=xc_send.at[which, k], recv_sem=xc_recv.at[which, k],
                device_id={"graph": peer}, device_id_type=MESH)

        def start(k, _):
            copy(k).start()
            return 0

        def wait(k, _):
            copy(k).wait()
            return 0

        return (lambda: lax.fori_loop(1, graph, start, 0)), (lambda: lax.fori_loop(1, graph, wait, 0))

    def block(ref, size):
        return lambda i: ref.at[pl.ds(pl.multiple_of(i * size, size), size)]

    def piece(ref, j, size):
        return lambda i: ref.at[j, pl.ds(pl.multiple_of(i * size, size), size)]

    def tiles(step):
        def one(i, _):
            step(pl.ds(pl.multiple_of(i * tile, tile), tile))
            return 0

        lax.fori_loop(0, triplets // tile, one, 0)

    def in_part(at):
        return one_hot(slot_total, in_ref[:, at])

    def out_part(at):
        return one_hot(slot_total, jnp.where(live_ref[:, at] > 0, out_ref[:, at], -1))

    def angles(at):
        angle[:, at] = lax.dot_general(
            bw_ref[...], basis_ref[:, at], (((0,), (0,)), ((), ())),
            precision=lax.Precision.HIGHEST, preferred_element_type=f32)

    part_a[...] = dot(state_ref[...], down_ref[...]).astype(bf16)
    for i in range(graph):
        lists_flat[:, i * cap:(i + 1) * cap] = lists_ref[0, i:i + 1, :]
    list_hot[...] = one_hot(rows, lists_flat[...])
    pl.semaphore_wait(barrier, graph - 1 + len(bits))
    mp_sum(0, part_a, got_a, sum_a, more_a, full_a, lambda: tiles(angles))

    step_rows = min(slot_total, 512)
    own = pl.ds(pl.multiple_of(g * cap, cap), cap)

    def pick(i, _):
        at = pl.ds(pl.multiple_of(i * step_rows, step_rows), step_rows)
        picked = dot(list_hot[:, at], full_a[...], 0, 0).astype(bf16)
        for j in range(pieces):
            to_a[j, at, :] = picked[:, j * lane:(j + 1) * lane]
        return 0

    lax.fori_loop(0, slot_total // step_rows, pick, 0)
    going = [exchange(j, piece(to_a, j, cap), from_a, piece(from_a, j, cap), cap) for j in range(pieces)]
    back = [exchange(pieces + j, piece(to_b, j, cap), from_b, piece(from_b, j, cap), cap) for j in range(pieces)]
    for start, _ in going:
        start()
    for j in range(pieces):
        from_a[j, own] = to_a[j, own]
    if kept:
        def keep(at):
            in_hot[:, at] = in_part(at)
            out_hot[:, at] = out_part(at)

        tiles(keep)

    for j in range(pieces):
        going[j][1]()
        slots[...] = jnp.zeros_like(slots)
        received = from_a[j].astype(f32).T.astype(bf16)

        def trips(at):
            source = in_hot[:, at] if kept else in_part(at)
            value = dot(received, source) * angle[j * lane:(j + 1) * lane, at]
            target = out_hot[:, at] if kept else out_part(at)
            slots[...] += dot(target, value.astype(bf16), 1, 1)

        tiles(trips)
        to_b[j] = slots[...].astype(bf16)
        back[j][0]()
        from_b[j, own] = to_b[j, own]

    for j in range(pieces):
        back[j][1]()
        part_b[:, j * lane:(j + 1) * lane] = dot(list_hot[...], from_b[j]).astype(bf16)

    plan, held = gather_plan(mp)
    order = [h * len(subs) + i for i in subs for h in (0, 1)]

    def other_of(off):
        index = m
        for bit in bits:
            if off & bit:
                index = flip(index, bit)
        return index

    def act_copy(layer, c, which):
        bit, off = plan[which]
        at = acts.at[layer, other_of(off), pl.ds(c * size, size)]
        return pltpu.make_async_remote_copy(
            src_ref=at, dst_ref=at,
            send_sem=act_send.at[layer, c, which], recv_sem=act_recv.at[layer, c, which],
            device_id={"mp": flip(m, bit)}, device_id_type=MESH)

    local = [i for i, (bit, off) in enumerate(plan) if off == 0]
    relayed = [i for i, (bit, off) in enumerate(plan) if off != 0]
    brings = {bit ^ off: i for i, (bit, off) in enumerate(plan)}
    relays_from = sorted({brings[plan[i][1]] for i in relayed})

    def send(layer, c):
        for i in local:
            act_copy(layer, c, i).start()

    def relay(layer, c):
        for i in relayed:
            first = brings[plan[i][1]]
            if [j for j in relayed if brings[plan[j][1]] == first][0] == i:
                act_copy(layer, c, first).wait_recv()
            act_copy(layer, c, i).start()

    def finish(layer, c):
        for i in range(len(plan)):
            if i not in relays_from:
                act_copy(layer, c, i).wait_recv()

    def begin(i):
        for c in order[2 * i:2 * i + 2]:
            at = pl.ds(c * size, size)
            first = state_ref[at, :].astype(f32) + dot(full_b[at, :], up_ref[...])
            hidden[at, :] = first
            acts[0, m, at, :] = first.astype(bf16)
            send(0, c)

    mp_sum(1, part_b, got_b, sum_b, more_b, full_b, ready=begin)
    load.wait()
    relay(0, order[0])

    def layer_step(l, _):
        for inside in range(2):
            k = 2 * l + inside
            for spot, c in enumerate(order):
                at = pl.ds(c * size, size)
                if spot + 1 < CHUNKS:
                    relay(k, order[spot + 1])
                elif inside == 0:
                    relay(k + 1, order[0])
                else:
                    @pl.when(l + 1 < layers)
                    def _():
                        relay(k + 1, order[0])
                finish(k, c)
                total = None
                for off in held:
                    index = other_of(off)
                    term = dot(acts[k, index, at, :], weight[k, pl.ds(pl.multiple_of(index * width, width), width), :])
                    total = term if total is None else total + term
                value = silu(total)
                if inside == 0:
                    acts[k + 1, m, at, :] = value.astype(bf16)
                    send(k + 1, c)
                else:
                    value = (hidden[at, :] + value) * inv_root_two
                    hidden[at, :] = value

                    @pl.when(l + 1 < layers)
                    def _():
                        acts[k + 1, m, at, :] = value.astype(bf16)
                        send(k + 1, c)
        return 0

    lax.fori_loop(0, layers, layer_step, 0)

    atom_rows = min(atoms, 256)

    def collect(i, _):
        at = pl.ds(pl.multiple_of(i * atom_rows, atom_rows), atom_rows)
        ids = one_hot(atom_rows, atom_ref[...] - i * atom_rows)
        high = hidden[...].astype(bf16)
        low = (hidden[...] - high.astype(f32)).astype(bf16)
        total = dot(ids, high) + dot(ids, low)
        atoms_own[at, :] = total
        atoms_to[at, :] = total.astype(bf16)
        return 0

    lax.fori_loop(0, atoms // atom_rows, collect, 0)
    start, wait = exchange(2 * pieces, block(atoms_to, ATOM_DEV), atoms_from, block(atoms_from, ATOM_DEV), ATOM_DEV)
    start()
    here = pl.ds(pl.multiple_of(g * ATOM_DEV, ATOM_DEV), ATOM_DEV)
    atoms_from[here] = jnp.zeros((ATOM_DEV, width), bf16)
    wait()

    def add(i, total):
        return total + atoms_from[pl.ds(pl.multiple_of(i * ATOM_DEV, ATOM_DEV), ATOM_DEV)].astype(f32)

    total = lax.fori_loop(0, graph, add, atoms_own[here])
    mine_out = silu(atom_scale * total).astype(bf16)
    table[here] = mine_out
    atom_out_ref[...] = mine_out
    start, wait = exchange(2 * pieces + 1, lambda peer: block(table, ATOM_DEV)(g), table, block(table, ATOM_DEV), ATOM_DEV)
    start()

    def drain(k, _):
        for c in range(CHUNKS):
            for i in range(len(plan)):
                act_copy(k, c, i).wait_send()
        return 0

    lax.fori_loop(0, 2 * layers, drain, 0)
    wait()

    def spread(i, _):
        at = pl.ds(pl.multiple_of(i * atom_rows, atom_rows), atom_rows)
        hidden[...] += dot(one_hot(atom_rows, atom_ref[...] - i * atom_rows), table[at, :], 0, 0)
        return 0

    lax.fori_loop(0, atoms // atom_rows, spread, 0)
    edge_out_ref[...] = hidden[...].astype(bf16)


def local(graph, mp, edge_state, down_weight, basis, basis_weight, up_weight, dense_weight,
          send_rows, trip_in, trip_out, trip_live, edge_atom):
    rows, width = edge_state.shape
    trip = down_weight.shape[1]
    slot_total = graph * send_rows.shape[2]
    triplets = trip_in.shape[0]
    maps = dense_weight.shape[0] * dense_weight.shape[1]
    tile = 512 if slot_total <= 512 else 128
    atoms = graph * ATOM_DEV
    stages = mp.bit_length()
    extra = max(stages - 2, 1)
    half = rows // 2
    vmem = pltpu.VMEM
    pieces = trip // 128 if trip % 128 == 0 else 1
    hot_bytes = 2 * 2 * slot_total * triplets
    hots = [vmem((slot_total, triplets), bf16)] * 2 if hot_bytes <= 2 ** 24 else [None, None]
    reduce_bufs = [
        vmem((rows, trip), bf16), vmem((half, trip), bf16), vmem((extra, half, trip), bf16),
        vmem((extra, half, trip), bf16), vmem((rows, trip), bf16),
    ]
    dma = pltpu.SemaphoreType.DMA
    spec = pl.BlockSpec(memory_space=pltpu.VMEM)
    body = functools.partial(kernel, graph, mp, tile)
    if hots[0] is None:
        hots, kept_body, at = [], body, 37
        body = lambda *refs: kept_body(*refs[:at], None, None, *refs[at:])
    return pl.pallas_call(
        body,
        out_shape=(
            jax.ShapeDtypeStruct((rows, width), bf16),
            jax.ShapeDtypeStruct((ATOM_DEV, width), bf16),
        ),
        in_specs=[spec] * 5 + [pl.BlockSpec(memory_space=pl.ANY)] + [spec] * 5,
        out_specs=(spec, spec),
        scratch_shapes=[
            vmem((maps,) + dense_weight.shape[2:], bf16), dma(()),
            *reduce_bufs, *reduce_bufs,
            dma((2, stages, CHUNKS // 2)), dma((2, stages, CHUNKS // 2)),
            *[vmem((pieces, slot_total, trip // pieces), bf16)] * 4,
            dma((2 * pieces + 2, graph)), dma((2 * pieces + 2, graph)),
            vmem((1, slot_total), jnp.int32), vmem((rows, slot_total), bf16),
            vmem((trip, triplets), f32), vmem((slot_total, trip // pieces), f32), *hots,
            vmem((maps, mp, rows, width), bf16), vmem((rows, max(width, trip)), f32),
            dma((maps, CHUNKS, mp - 1)), dma((maps, CHUNKS, mp - 1)),
            vmem((atoms, width), f32), vmem((atoms, width), bf16), vmem((atoms, width), bf16),
            vmem((atoms, width), bf16),
        ],
        compiler_params=pltpu.CompilerParams(
            collective_id=0, has_side_effects=True, vmem_limit_bytes=64000 * 1024
        ),
        name="edge_block",
    )(
        edge_state, down_weight, basis, basis_weight, up_weight,
        dense_weight.reshape((maps,) + dense_weight.shape[2:]),
        send_rows, trip_in.reshape(1, triplets), trip_out.reshape(1, triplets),
        trip_live.reshape(1, triplets), edge_atom.reshape(1, rows),
    )


def solution(mesh):
    in_specs = (
        P("graph", "mp"),
        P("mp", None),
        P(None, ("graph", "mp")),
        P(),
        P(None, "mp"),
        P(None, None, None, "mp"),
        P("graph", "mp", None),
        P(("graph", "mp")),
        P(("graph", "mp")),
        P(("graph", "mp")),
        P("graph"),
    )
    out_specs = (P("graph", "mp"), P("graph", "mp"))
    body = functools.partial(local, mesh.shape["graph"], mesh.shape["mp"])
    return jax.shard_map(body, mesh=mesh, in_specs=in_specs, out_specs=out_specs, check_vma=False)
```

```python
import functools

import jax
import jax.numpy as jnp
from jax import lax
from jax.experimental import pallas as pl
from jax.experimental.pallas import tpu as pltpu
from jax.sharding import PartitionSpec as P

ATOM_DEV = 32
CHUNKS = 4

inv_root_two = 0.7071067811865476
atom_scale = 0.2

MESH = pl.DeviceIdType.MESH
bf16 = jnp.bfloat16
f32 = jnp.float32


def silu(v):
    return v / (1.0 + jnp.exp(-v))


def flip(index, bit):
    return index + bit - 2 * bit * ((index // bit) % 2)


def one_hot(rows, ids):
    shape = (rows, ids.shape[1])
    return jnp.where(lax.broadcasted_iota(jnp.int32, shape, 0) == ids, 1.0, 0.0).astype(bf16)


def dot(a, b, ca=1, cb=0):
    return lax.dot_general(a, b, (((ca,), (cb,)), ((), ())), preferred_element_type=f32)


def gather_plan(mp):
    plan, held, bit = [], [0], mp // 2
    while bit >= 1:
        plan += [(bit, off) for off in held]
        held += [bit ^ off for off in held]
        bit //= 2
    return plan, held


def kernel(
    graph, mp, tile,
    state_ref, down_ref, basis_ref, bw_ref, up_ref, dense_hbm, lists_ref, in_ref, out_ref, live_ref, atom_ref,
    edge_out_ref, atom_out_ref,
    weight, weight_sem,
    part_a, got_a, sum_a, more_a, full_a,
    part_b, got_b, sum_b, more_b, full_b,
    red_send, red_recv,
    to_a, from_a, to_b, from_b, xc_send, xc_recv,
    lists_flat, list_hot, angle, slots, in_hot, out_hot,
    acts, hidden, act_send, act_recv,
    atoms_own, atoms_to, atoms_from, table,
):
    g = lax.axis_index("graph")
    m = lax.axis_index("mp")
    rows, width = state_ref.shape
    trip = down_ref.shape[1]
    layers = weight.shape[0] // 2
    cap = lists_ref.shape[2]
    slot_total = graph * cap
    pieces, lane = to_a.shape[0], to_a.shape[2]
    kept = in_hot is not None
    triplets = in_ref.shape[1]
    atoms = graph * ATOM_DEV
    half = rows // 2
    bits = [1 << i for i in range(mp.bit_length() - 1)]

    load = pltpu.make_async_copy(dense_hbm, weight, weight_sem)
    load.start()

    barrier = pltpu.get_barrier_semaphore()

    def greet(k, _):
        pl.semaphore_signal(barrier, inc=1, device_id={"graph": (g + k) % graph}, device_id_type=MESH)
        return 0

    lax.fori_loop(1, graph, greet, 0)
    for bit in bits:
        pl.semaphore_signal(barrier, inc=1, device_id={"mp": flip(m, bit)}, device_id_type=MESH)

    def mp_copy(src, dst, which, slot, i, bit):
        return pltpu.make_async_remote_copy(
            src_ref=src, dst_ref=dst, send_sem=red_send.at[which, slot, i], recv_sem=red_recv.at[which, slot, i],
            device_id={"mp": flip(m, bit)}, device_id_type=MESH)

    mine = pl.multiple_of((m % 2) * half, half)
    other = pl.multiple_of(half - (m % 2) * half, half)
    size = rows // CHUNKS
    subs = range(CHUNKS // 2)

    def mp_sum(which, part, got, summed, more, full, meanwhile=None, ready=None):
        at = [pl.ds(i * size, size) for i in subs]
        firsts = [mp_copy(part.at[pl.ds(other + i * size, size)], got.at[at[i]], which, 0, i, 1) for i in subs]
        steps = [[mp_copy(summed.at[b, at[i]], more.at[b, at[i]], which, 1 + b, i, bit) for i in subs]
                 for b, bit in enumerate(bits[1:])]
        for first in firsts:
            first.start()

        def total(b, i):
            if b == 0:
                return part[pl.ds(mine + i * size, size)].astype(f32) + got[at[i]].astype(f32)
            return summed[b - 1, at[i]].astype(f32) + more[b - 1, at[i]].astype(f32)

        for b in range(len(bits) - 1):
            for i in subs:
                (firsts[i] if b == 0 else steps[b - 1][i]).wait()
                summed[b, at[i]] = total(b, i).astype(bf16)
                steps[b][i].start()
        if meanwhile is not None:
            meanwhile()
        lasts = []
        for i in subs:
            (firsts[i] if len(bits) == 1 else steps[-1][i]).wait()
            here = pl.ds(mine + i * size, size)
            full[here] = total(len(bits) - 1, i).astype(bf16)
            lasts.append(mp_copy(full.at[here], full.at[here], which, len(bits), i, 1))
            lasts[i].start()
            if ready is not None:
                lasts[i].wait()
                ready(i)
        if ready is None:
            for last in lasts:
                last.wait()

    def exchange(which, src_at, dst, dst_at, size):
        def copy(k):
            peer = (g + k) % graph
            return pltpu.make_async_remote_copy(
                src_ref=src_at(peer), dst_ref=dst_at(g),
                send_sem=xc_send.at[which, k], recv_sem=xc_recv.at[which, k],
                device_id={"graph": peer}, device_id_type=MESH)

        def start(k, _):
            copy(k).start()
            return 0

        def wait(k, _):
            copy(k).wait()
            return 0

        return (lambda: lax.fori_loop(1, graph, start, 0)), (lambda: lax.fori_loop(1, graph, wait, 0))

    def block(ref, size):
        return lambda i: ref.at[pl.ds(pl.multiple_of(i * size, size), size)]

    def piece(ref, j, size):
        return lambda i: ref.at[j, pl.ds(pl.multiple_of(i * size, size), size)]

    def tiles(step):
        def one(i, _):
            step(pl.ds(pl.multiple_of(i * tile, tile), tile))
            return 0

        lax.fori_loop(0, triplets // tile, one, 0)

    def in_part(at):
        return one_hot(slot_total, in_ref[:, at])

    def out_part(at):
        return one_hot(slot_total, jnp.where(live_ref[:, at] > 0, out_ref[:, at], -1))

    def angles(at):
        angle[:, at] = lax.dot_general(
            bw_ref[...], basis_ref[:, at], (((0,), (0,)), ((), ())),
            precision=lax.Precision.HIGHEST, preferred_element_type=f32)

    part_a[...] = dot(state_ref[...], down_ref[...]).astype(bf16)
    for i in range(graph):
        lists_flat[:, i * cap:(i + 1) * cap] = lists_ref[0, i:i + 1, :]
    list_hot[...] = one_hot(rows, lists_flat[...])
    pl.semaphore_wait(barrier, graph - 1 + len(bits))
    mp_sum(0, part_a, got_a, sum_a, more_a, full_a, lambda: tiles(angles))

    step_rows = min(slot_total, 512)
    own = pl.ds(pl.multiple_of(g * cap, cap), cap)

    def pick(i, _):
        at = pl.ds(pl.multiple_of(i * step_rows, step_rows), step_rows)
        picked = dot(list_hot[:, at], full_a[...], 0, 0).astype(bf16)
        for j in range(pieces):
            to_a[j, at, :] = picked[:, j * lane:(j + 1) * lane]
        return 0

    lax.fori_loop(0, slot_total // step_rows, pick, 0)
    going = [exchange(j, piece(to_a, j, cap), from_a, piece(from_a, j, cap), cap) for j in range(pieces)]
    back = [exchange(pieces + j, piece(to_b, j, cap), from_b, piece(from_b, j, cap), cap) for j in range(pieces)]
    for start, _ in going:
        start()
    for j in range(pieces):
        from_a[j, own] = to_a[j, own]
    if kept:
        def keep(at):
            in_hot[:, at] = in_part(at)
            out_hot[:, at] = out_part(at)

        tiles(keep)

    for j in range(pieces):
        going[j][1]()
        slots[...] = jnp.zeros_like(slots)
        received = from_a[j].astype(f32).T.astype(bf16)

        def trips(at):
            source = in_hot[:, at] if kept else in_part(at)
            value = dot(received, source) * angle[j * lane:(j + 1) * lane, at]
            target = out_hot[:, at] if kept else out_part(at)
            slots[...] += dot(target, value.astype(bf16), 1, 1)

        tiles(trips)
        to_b[j] = slots[...].astype(bf16)
        back[j][0]()
        from_b[j, own] = to_b[j, own]

    for j in range(pieces):
        back[j][1]()
        part_b[:, j * lane:(j + 1) * lane] = dot(list_hot[...], from_b[j]).astype(bf16)

    plan, held = gather_plan(mp)
    order = [h * len(subs) + i for i in subs for h in (0, 1)]

    def other_of(off):
        index = m
        for bit in bits:
            if off & bit:
                index = flip(index, bit)
        return index

    def act_copy(layer, c, which):
        bit, off = plan[which]
        at = acts.at[layer, other_of(off), pl.ds(c * size, size)]
        return pltpu.make_async_remote_copy(
            src_ref=at, dst_ref=at,
            send_sem=act_send.at[layer, c, which], recv_sem=act_recv.at[layer, c, which],
            device_id={"mp": flip(m, bit)}, device_id_type=MESH)

    local = [i for i, (bit, off) in enumerate(plan) if off == 0]
    relayed = [i for i, (bit, off) in enumerate(plan) if off != 0]
    brings = {bit ^ off: i for i, (bit, off) in enumerate(plan)}
    relays_from = sorted({brings[plan[i][1]] for i in relayed})

    def send(layer, c):
        for i in local:
            act_copy(layer, c, i).start()

    def relay(layer, c):
        for i in relayed:
            first = brings[plan[i][1]]
            if [j for j in relayed if brings[plan[j][1]] == first][0] == i:
                act_copy(layer, c, first).wait_recv()
            act_copy(layer, c, i).start()

    def finish(layer, c):
        for i in range(len(plan)):
            if i not in relays_from:
                act_copy(layer, c, i).wait_recv()

    def begin(i):
        for c in order[2 * i:2 * i + 2]:
            at = pl.ds(c * size, size)
            first = state_ref[at, :].astype(f32) + dot(full_b[at, :], up_ref[...])
            hidden[at, :] = first
            acts[0, m, at, :] = first.astype(bf16)
            send(0, c)

    mp_sum(1, part_b, got_b, sum_b, more_b, full_b, ready=begin)
    load.wait()
    relay(0, order[0])

    def layer_step(l, _):
        for inside in range(2):
            k = 2 * l + inside
            for spot, c in enumerate(order):
                at = pl.ds(c * size, size)
                if spot + 1 < CHUNKS:
                    relay(k, order[spot + 1])
                elif inside == 0:
                    relay(k + 1, order[0])
                else:
                    @pl.when(l + 1 < layers)
                    def _():
                        relay(k + 1, order[0])
                finish(k, c)
                total = None
                for off in held:
                    index = other_of(off)
                    term = dot(acts[k, index, at, :], weight[k, pl.ds(pl.multiple_of(index * width, width), width), :])
                    total = term if total is None else total + term
                value = silu(total)
                if inside == 0:
                    acts[k + 1, m, at, :] = value.astype(bf16)
                    send(k + 1, c)
                else:
                    value = (hidden[at, :] + value) * inv_root_two
                    hidden[at, :] = value

                    @pl.when(l + 1 < layers)
                    def _():
                        acts[k + 1, m, at, :] = value.astype(bf16)
                        send(k + 1, c)
        return 0

    lax.fori_loop(0, layers, layer_step, 0)

    atom_rows = min(atoms, 256)

    def collect(i, _):
        at = pl.ds(pl.multiple_of(i * atom_rows, atom_rows), atom_rows)
        ids = one_hot(atom_rows, atom_ref[...] - i * atom_rows)
        high = hidden[...].astype(bf16)
        low = (hidden[...] - high.astype(f32)).astype(bf16)
        total = dot(ids, high) + dot(ids, low)
        atoms_own[at, :] = total
        atoms_to[at, :] = total.astype(bf16)
        return 0

    lax.fori_loop(0, atoms // atom_rows, collect, 0)
    start, wait = exchange(2 * pieces, block(atoms_to, ATOM_DEV), atoms_from, block(atoms_from, ATOM_DEV), ATOM_DEV)
    start()
    here = pl.ds(pl.multiple_of(g * ATOM_DEV, ATOM_DEV), ATOM_DEV)
    atoms_from[here] = jnp.zeros((ATOM_DEV, width), bf16)
    wait()

    def add(i, total):
        return total + atoms_from[pl.ds(pl.multiple_of(i * ATOM_DEV, ATOM_DEV), ATOM_DEV)].astype(f32)

    total = lax.fori_loop(0, graph, add, atoms_own[here])
    mine_out = silu(atom_scale * total).astype(bf16)
    table[here] = mine_out
    atom_out_ref[...] = mine_out
    start, wait = exchange(2 * pieces + 1, lambda peer: block(table, ATOM_DEV)(g), table, block(table, ATOM_DEV), ATOM_DEV)
    start()

    def drain(k, _):
        for c in range(CHUNKS):
            for i in range(len(plan)):
                act_copy(k, c, i).wait_send()
        return 0

    lax.fori_loop(0, 2 * layers, drain, 0)
    wait()

    def spread(i, _):
        at = pl.ds(pl.multiple_of(i * atom_rows, atom_rows), atom_rows)
        hidden[...] += dot(one_hot(atom_rows, atom_ref[...] - i * atom_rows), table[at, :], 0, 0)
        return 0

    lax.fori_loop(0, atoms // atom_rows, spread, 0)
    edge_out_ref[...] = hidden[...].astype(bf16)


def hand_on(edge_ref, atom_ref, edge_out_ref, atom_out_ref):
    edge_out_ref[...] = edge_ref[...]
    atom_out_ref[...] = atom_ref[...]


def local(graph, mp, edge_state, down_weight, basis, basis_weight, up_weight, dense_weight,
          send_rows, trip_in, trip_out, trip_live, edge_atom):
    rows, width = edge_state.shape
    trip = down_weight.shape[1]
    slot_total = graph * send_rows.shape[2]
    triplets = trip_in.shape[0]
    maps = dense_weight.shape[0] * dense_weight.shape[1]
    tile = 2048 if slot_total <= 512 else 128
    atoms = graph * ATOM_DEV
    stages = mp.bit_length()
    extra = max(stages - 2, 1)
    half = rows // 2
    vmem = pltpu.VMEM
    pieces = trip // 128 if trip % 128 == 0 else 1
    hot_bytes = 2 * 2 * slot_total * triplets
    hots = [vmem((slot_total, triplets), bf16)] * 2 if hot_bytes <= 2 ** 24 else [None, None]
    reduce_bufs = [
        vmem((rows, trip), bf16), vmem((half, trip), bf16), vmem((extra, half, trip), bf16),
        vmem((extra, half, trip), bf16), vmem((rows, trip), bf16),
    ]
    dma = pltpu.SemaphoreType.DMA
    spec = pl.BlockSpec(memory_space=pltpu.VMEM)
    body = functools.partial(kernel, graph, mp, tile)
    if hots[0] is None:
        hots, kept_body, at = [], body, 37
        body = lambda *refs: kept_body(*refs[:at], None, None, *refs[at:])
    outs = pl.pallas_call(
        body,
        out_shape=(
            jax.ShapeDtypeStruct((rows, width), bf16),
            jax.ShapeDtypeStruct((ATOM_DEV, width), bf16),
        ),
        in_specs=[spec] * 5 + [pl.BlockSpec(memory_space=pl.ANY)] + [spec] * 5,
        out_specs=(spec, spec),
        scratch_shapes=[
            vmem((maps,) + dense_weight.shape[2:], bf16), dma(()),
            *reduce_bufs, *reduce_bufs,
            dma((2, stages, CHUNKS // 2)), dma((2, stages, CHUNKS // 2)),
            *[vmem((pieces, slot_total, trip // pieces), bf16)] * 4,
            dma((2 * pieces + 2, graph)), dma((2 * pieces + 2, graph)),
            vmem((1, slot_total), jnp.int32), vmem((rows, slot_total), bf16),
            vmem((trip, triplets), f32), vmem((slot_total, trip // pieces), f32), *hots,
            vmem((maps, mp, rows, width), bf16), vmem((rows, max(width, trip)), f32),
            dma((maps, CHUNKS, mp - 1)), dma((maps, CHUNKS, mp - 1)),
            vmem((atoms, width), f32), vmem((atoms, width), bf16), vmem((atoms, width), bf16),
            vmem((atoms, width), bf16),
        ],
        compiler_params=pltpu.CompilerParams(
            collective_id=0, has_side_effects=True, vmem_limit_bytes=64000 * 1024
        ),
        name="edge_block",
    )(
        edge_state, down_weight, basis, basis_weight, up_weight,
        dense_weight.reshape((maps,) + dense_weight.shape[2:]),
        send_rows, trip_in.reshape(1, triplets), trip_out.reshape(1, triplets),
        trip_live.reshape(1, triplets), edge_atom.reshape(1, rows),
    )
    return pl.pallas_call(
        hand_on,
        out_shape=tuple(jax.ShapeDtypeStruct(o.shape, o.dtype) for o in outs),
        in_specs=[spec] * 2,
        out_specs=(spec, spec),
        name="hand_on",
    )(*outs)


def solution(mesh):
    in_specs = (
        P("graph", "mp"),
        P("mp", None),
        P(None, ("graph", "mp")),
        P(),
        P(None, "mp"),
        P(None, None, None, "mp"),
        P("graph", "mp", None),
        P(("graph", "mp")),
        P(("graph", "mp")),
        P(("graph", "mp")),
        P("graph"),
    )
    out_specs = (P("graph", "mp"), P("graph", "mp"))
    body = functools.partial(local, mesh.shape["graph"], mesh.shape["mp"])
    return jax.shard_map(body, mesh=mesh, in_specs=in_specs, out_specs=out_specs, check_vma=False)
```
